32 devices in a mesh: shard: 8 (over z, x), tp: 4 (over y, core).
Axes of the slice: x: 2, y: 2, z: 4, core: 2. Of those that a mesh axis runs over, the one named last changes fastest.
Arguments:
- one_gate: float32 [2048, 8192], P('shard', 'tp'), may hold values from -0.1875 to 0.1875
- other_gate: float32 [2048, 8192], P('shard', 'tp'), may hold values from -0.125 to 0.125
- one_up: float32 [2048, 8192], P('shard', 'tp'), may hold values from -0.1875 to 0.1875
- other_up: float32 [2048, 8192], P('shard', 'tp'), may hold values from -0.125 to 0.125
- mix_share: float32 [2048], P('shard'), may hold values from 0.2 to 0.8
- norm_train: float32 [2048], P(('shard', 'tp')), may hold values from 0.25 to 1.75
- norm_step: float32 [2048], P(('shard', 'tp')), may hold values from -0.3 to 0.3
Outputs:
- serve_gate: bfloat16 [2048, 8192], P(None, 'tp')
- serve_up: bfloat16 [2048, 8192], P(None, 'tp')
- factor_gate: float32 [8192], P('tp')
- factor_up: float32 [8192], P('tp')
- serve_norm: bfloat16 [2048], replicated
The draws below stay inside these ranges and needn't reach their ends.
All inputs are finite; a program needn't handle non-finite values.
Results may differ from the reference program's by a relative error of at most 0.0004.
Values may be sent and summed in bfloat16 or wider, within the bound.
No kernel may reach another device: no remote copies, remote signals or barrier semaphores. Data moves between devices by JAX's collectives and lax.ppermute only.
A program may use at most 128 MiB of HBM per device.

```python
import jax
import jax.numpy as jnp
from jax import lax

D_MODEL = 2048
D_INNER = 8192


def with_spikes(array, key, source, target, blocks, factor):
    owner, partner = [(jnp.arange(array.shape[axis_at]) // (array.shape[axis_at] // blocks)).reshape([-1 if axis == axis_at else 1 for axis in range(array.ndim)]) for axis_at in (source, target)]
    chosen = jax.random.permutation(key, blocks)[partner]
    strong = (owner == chosen) | (owner == (partner + blocks // 2) % blocks)
    return jnp.where(strong, factor * array, array)


def shard_levels(key, shape, pieces, low, largest):
    level = 1.0
    for axis_at, shards_of in pieces:
        draws = jax.random.uniform(jax.random.fold_in(jax.random.fold_in(key, 6), axis_at), (shards_of,), jnp.float32, low / len(pieces), largest / len(pieces))
        level = level * jnp.repeat(jnp.exp(draws), shape[axis_at] // shards_of).reshape((-1,) + (1,) * (len(shape) - 1 - axis_at))
    return level


def normal_values(stream_key, extent, width, bound, split=(), kind=jnp.bfloat16):
    level = shard_levels(stream_key, extent, split, -0.22, 0.18) if split else 1.0
    values = jax.random.normal(stream_key, extent, jnp.float32) * width * level
    return jnp.minimum(jnp.maximum(values, -bound), bound).astype(kind)


def bell_draw_with(own_key, shape, width, most, split, heavy, held_as=jnp.bfloat16):
    result = width * jax.random.normal(own_key, shape, jnp.float32)
    if split:
        result = result * shard_levels(own_key, shape, split, -0.22, 0.18)
    return jnp.clip(with_spikes(result, jax.random.fold_in(own_key, 3), *heavy), -most, most).astype(held_as)


def setup_inputs(seed: int = 0) -> dict:
    arg_keys = jax.random.split(jax.random.key(seed), 8)
    one_gate = bell_draw_with(arg_keys[0], (D_MODEL, D_INNER), D_MODEL ** -0.5, 0.1875, ((0, 8), (1, 4)), (0, 1, 8, 2.0), jnp.float32)
    other_gate = normal_values(arg_keys[1], (D_MODEL, D_INNER), D_MODEL ** -0.5, 0.125, ((0, 8), (1, 4)), jnp.float32)
    one_up = bell_draw_with(arg_keys[2], (D_MODEL, D_INNER), D_MODEL ** -0.5, 0.1875, ((0, 8), (1, 4)), (0, 1, 8, 2.0), jnp.float32)
    other_up = normal_values(arg_keys[3], (D_MODEL, D_INNER), D_MODEL ** -0.5, 0.125, ((0, 8), (1, 4)), jnp.float32)
    mix_share = jnp.clip(0.2 + 0.6 * jax.random.uniform(arg_keys[4], (D_MODEL,), jnp.float32) ** shard_levels(arg_keys[4], (D_MODEL,), ((0, 8),), -0.2, 0.2), 0.2, 0.8)
    norm_train = jnp.clip(1.0 + 0.15 * jax.random.normal(arg_keys[5], (D_MODEL,), jnp.float32), 0.25, 1.75)
    norm_step = jnp.clip(jax.random.uniform(arg_keys[6], (D_MODEL,), jnp.float32, -0.3, 0.3) * shard_levels(arg_keys[6], (D_MODEL,), ((0, 32),), -0.4, 0.0), -0.3, 0.3)
    return dict(one_gate=one_gate, other_gate=other_gate, one_up=one_up, other_up=other_up, mix_share=mix_share, norm_train=norm_train, norm_step=norm_step)


def reference(one_gate, other_gate, one_up, other_up, mix_share, norm_train, norm_step):
    fresh_gate = mix_share[:, None] * one_gate + (1.0 - mix_share[:, None]) * other_gate
    fresh_up = mix_share[:, None] * one_up + (1.0 - mix_share[:, None]) * other_up
    factor_gate = jnp.sqrt(lax.optimization_barrier(jnp.sum(fresh_gate * fresh_gate, axis=0)))
    serve_gate = (fresh_gate / factor_gate).astype(jnp.bfloat16)
    factor_up = jnp.sqrt(lax.optimization_barrier(jnp.sum(fresh_up * fresh_up, axis=0)))
    serve_up = (fresh_up / factor_up).astype(jnp.bfloat16)
    serve_norm = (norm_train + norm_step).astype(jnp.bfloat16)
    return (serve_gate, serve_up, factor_gate, factor_up, serve_norm)
```

```python
import functools

import jax
import jax.numpy as jnp
from jax import lax
from jax.experimental import pallas as pl
from jax.experimental.pallas import tpu as pltpu
from jax.sharding import PartitionSpec as P

CHUNKS = 2


def ring_order(n):
    return list(range(0, n, 2)) + list(range(1, n, 2))[::-1]


def place_kernel(index_ref, one_g, other_g, one_u, other_u, share, root_g, root_u, out_g, out_u, narrow_g, narrow_u):
    mix = share[...]
    rest = 1.0 - mix
    gate = ((mix * one_g[...] + rest * other_g[...]) / root_g[...]).astype(jnp.bfloat16)
    up = ((mix * one_u[...] + rest * other_u[...]) / root_u[...]).astype(jnp.bfloat16)
    out_g[...] = gate
    out_u[...] = up
    narrow_g[...] = gate
    narrow_u[...] = up


def place(index, one_gate, other_gate, one_up, other_up, share, root_gate, root_up, n):
    rows, cols = one_gate.shape
    tile = min(64, rows)
    steps = rows // tile
    wide = pl.BlockSpec((tile, cols), lambda i, index: (i, 0))
    column = pl.BlockSpec((tile, 1), lambda i, index: (i, 0))
    row = pl.BlockSpec((1, cols), lambda i, index: (0, 0))
    placed = pl.BlockSpec((tile, cols), lambda i, index: (index[0] * steps + i, 0))
    return pl.pallas_call(
        place_kernel,
        grid_spec=pltpu.PrefetchScalarGridSpec(
            num_scalar_prefetch=1,
            grid=(steps,),
            in_specs=[wide, wide, wide, wide, column, row, row],
            out_specs=[placed, placed, wide, wide],
        ),
        out_shape=[
            jax.ShapeDtypeStruct((n * rows, cols), jnp.bfloat16),
            jax.ShapeDtypeStruct((n * rows, cols), jnp.bfloat16),
            jax.ShapeDtypeStruct((rows, cols), jnp.bfloat16),
            jax.ShapeDtypeStruct((rows, cols), jnp.bfloat16),
        ],
        name="place",
    )(index, one_gate, other_gate, one_up, other_up, share, root_gate, root_up)


def shards(mesh, one_gate, other_gate, one_up, other_up, mix_share, norm_train, norm_step):
    n, t = mesh.shape["shard"], mesh.shape["tp"]
    me = lax.axis_index("shard")
    rows, cols = one_gate.shape
    order = ring_order(n)
    forward = [(order[i], order[(i + 1) % n]) for i in range(n)]
    backward = [(b, a) for a, b in forward]
    share = mix_share[:, None]
    fresh_gate = share * one_gate + (1.0 - share) * other_gate
    fresh_up = share * one_up + (1.0 - share) * other_up
    part = jnp.stack([jnp.sum(fresh_gate * fresh_gate, axis=0), jnp.sum(fresh_up * fresh_up, axis=0)])
    terms = [part] + [lax.ppermute(part, "shard", [(i, i ^ k) for i in range(n)]) for k in range(1, n)]
    while len(terms) > 1:
        terms = [terms[i] + terms[i + 1] for i in range(0, len(terms), 2)]
    root = jnp.sqrt(terms[0])
    factor_gate, factor_up = root[0], root[1]
    out_gate, out_up, gate, up = place(
        me[None].astype(jnp.int32), one_gate, other_gate, one_up, other_up, share, root[0:1], root[1:2], n
    )
    spot = jnp.where(me % 2 == 0, me // 2, n - 1 - me // 2)
    table = jnp.array(order, jnp.int32)
    piece = rows // CHUNKS
    held_gate = [gate[c * piece:(c + 1) * piece] for c in range(CHUNKS)]
    held_up = [up[c * piece:(c + 1) * piece] for c in range(CHUNKS)]
    for step in range(1, n):
        from_gate = table[(spot - step) % n]
        from_up = table[(spot + step) % n]
        for c in range(CHUNKS):
            held_gate[c] = lax.ppermute(held_gate[c], "shard", forward)
            held_up[c] = lax.ppermute(held_up[c], "shard", backward)
        for c in range(CHUNKS):
            out_gate = lax.dynamic_update_slice(out_gate, held_gate[c], (from_gate * rows + c * piece, 0))
            out_up = lax.dynamic_update_slice(out_up, held_up[c], (from_up * rows + c * piece, 0))
    width = norm_train.shape[0]
    norm = (norm_train + norm_step).astype(jnp.bfloat16)
    tp_index = lax.axis_index("tp")
    serve_norm = jnp.zeros((n * t * width,), jnp.bfloat16)
    serve_norm = lax.dynamic_update_slice(serve_norm, norm, ((me * t + tp_index) * width,))
    k = 1
    while k < t:
        serve_norm = serve_norm + lax.ppermute(serve_norm, "tp", [(i, i ^ k) for i in range(t)])
        k *= 2
    k = 1
    while k < n:
        serve_norm = serve_norm + lax.ppermute(serve_norm, "shard", [(i, i ^ k) for i in range(n)])
        k *= 2
    return (out_gate, out_up, factor_gate, factor_up, serve_norm)


def solution(mesh):
    return jax.shard_map(
        functools.partial(shards, mesh),
        mesh=mesh,
        in_specs=(
            P("shard", "tp"),
            P("shard", "tp"),
            P("shard", "tp"),
            P("shard", "tp"),
            P("shard"),
            P(("shard", "tp")),
            P(("shard", "tp")),
        ),
        out_specs=(P(None, "tp"), P(None, "tp"), P("tp"), P("tp"), P()),
        check_vma=False,
    )
```

```python
import functools

import jax
import jax.numpy as jnp
from jax import lax
from jax.experimental import pallas as pl
from jax.experimental.pallas import tpu as pltpu
from jax.sharding import PartitionSpec as P

WHOLE = pl.BlockSpec(memory_space=pltpu.VMEM)
OUTSIDE = pl.BlockSpec(memory_space=pl.ANY)
SCALARS = pl.BlockSpec(memory_space=pltpu.SMEM)


def grant(mib):
    return pltpu.CompilerParams(vmem_limit_bytes=mib << 20)


def ring_order(n):
    return list(range(0, n, 2)) + list(range(1, n, 2))[::-1]


def ring_neighbour(shard, distance, n):
    place = lax.rem(jnp.where(lax.rem(shard, 2) == 0, shard // 2, n - 1 - shard // 2) + distance + n, n)
    return jnp.where(place < n - n // 2, 2 * place, 2 * (n - 1 - place) + 1)


def cuts(rows):
    if rows < 256:
        return [(0, rows)]
    edges = [0, 5 * rows // 8, rows]
    return list(zip(edges[:-1], edges[1:]))


def sums_kernel(pieces, share, one_g, other_g, one_u, other_u, fresh_g, fresh_u, sums, held, shares, sems, share_sem):
    rows, cols = fresh_g.shape
    tall = rows // pieces
    sources = (one_g, other_g, one_u, other_u)

    def copy(k, p):
        span = pl.ds(p * tall, tall)
        return pltpu.make_async_copy(sources[k].at[span], held.at[k, span], sems.at[k, p])

    first = pltpu.make_async_copy(share, shares, share_sem)
    first.start()
    for p in range(pieces):
        for k in range(4):
            copy(k, p).start()
    first.wait()
    row = lax.broadcasted_iota(jnp.int32, (rows, rows), 0)
    lane = lax.broadcasted_iota(jnp.int32, (rows, rows), 1)
    mix = jnp.sum(jnp.where(row == lane, shares[...], 0.0), axis=1, keepdims=True)
    rest = 1.0 - mix
    total = [jnp.zeros((8, cols), jnp.float32) for _ in range(2)]
    for p in range(pieces):
        for k in range(4):
            copy(k, p).wait()
        for r in range(p * tall, (p + 1) * tall, 8):
            m, w = mix[r:r + 8], rest[r:r + 8]
            for side, fresh in ((0, fresh_g), (1, fresh_u)):
                value = m * held[2 * side, r:r + 8] + w * held[2 * side + 1, r:r + 8]
                fresh[r:r + 8] = value
                total[side] = total[side] + value * value
    sums[0:1] = jnp.sum(total[0], axis=0, keepdims=True)
    sums[1:2] = jnp.sum(total[1], axis=0, keepdims=True)


def sums_of(share, one_gate, other_gate, one_up, other_up):
    rows, cols = one_gate.shape
    pieces = max(1, rows // 32)
    wide = jax.ShapeDtypeStruct((rows, cols), jnp.float32)
    return pl.pallas_call(
        functools.partial(sums_kernel, pieces),
        in_specs=[OUTSIDE] * 5,
        out_specs=[WHOLE] * 3,
        out_shape=[wide, wide, jax.ShapeDtypeStruct((2, cols), jnp.float32)],
        scratch_shapes=[
            pltpu.VMEM((4, rows, cols), jnp.float32),
            pltpu.VMEM(share.shape, jnp.float32),
            pltpu.SemaphoreType.DMA((4, pieces)),
            pltpu.SemaphoreType.DMA,
        ],
        compiler_params=grant(48),
        name="sums",
    )(share, one_gate, other_gate, one_up, other_up)


def narrow_kernel(spans, fresh_g, fresh_u, total_ref, factor_g, factor_u, *outs):
    for side, fresh, factor in ((0, fresh_g, factor_g), (1, fresh_u, factor_u)):
        factor[...] = jnp.sqrt(total_ref[side:side + 1])
        scale = 1.0 / factor[...]
        for (lo, hi), out in zip(spans, outs[side * len(spans):]):
            for r in range(lo, hi, 16):
                out[r - lo:r - lo + 16] = (fresh[r:r + 16] * scale).astype(jnp.bfloat16)


def narrow(spans, fresh_gate, fresh_up, total):
    cols = fresh_gate.shape[1]
    factor = jax.ShapeDtypeStruct((1, cols), jnp.float32)
    shapes = [jax.ShapeDtypeStruct((hi - lo, cols), jnp.bfloat16) for lo, hi in spans]
    factor_gate, factor_up, *pieces = pl.pallas_call(
        functools.partial(narrow_kernel, spans),
        in_specs=[WHOLE] * 3,
        out_specs=[WHOLE] * (2 + 2 * len(spans)),
        out_shape=[factor] * 2 + shapes * 2,
        compiler_params=grant(16),
        name="narrow",
    )(fresh_gate, fresh_up, total)
    return factor_gate, factor_up, pieces[:len(spans)], pieces[len(spans):]


def run(copies):
    for copy in copies:
        copy.start()
    for copy in copies:
        copy.wait()


def start_kernel(spans, shard_ref, *refs):
    count = len(spans)
    outs, sems = refs[2 * count:2 * count + 2], refs[-1]
    first = pl.multiple_of(shard_ref[0] * spans[-1][1], 16)
    run([
        pltpu.make_async_copy(refs[side * count + c], outs[side].at[pl.ds(first + lo, hi - lo)], sems.at[side, c])
        for side in range(2)
        for c, (lo, hi) in enumerate(spans)
    ])


def start_outputs(shard, spans, gate, up, n):
    shape = jax.ShapeDtypeStruct((n * spans[-1][1], gate[0].shape[1]), jnp.bfloat16)
    return pl.pallas_call(
        functools.partial(start_kernel, spans),
        in_specs=[SCALARS] + [WHOLE] * (2 * len(spans)),
        out_specs=[OUTSIDE] * 2,
        out_shape=[shape, shape],
        scratch_shapes=[pltpu.SemaphoreType.DMA((2, len(spans)))],
        compiler_params=grant(4),
        name="start_outputs",
    )(shard, *gate, *up)


def put_kernel(step, lo, rows, n, shard_ref, gate, up, _, __, out_g, out_u, sems):
    copies = []
    for side, (part, out, back) in enumerate(((gate, out_g, -step), (up, out_u, step))):
        first = pl.multiple_of(ring_neighbour(shard_ref[0], back, n) * rows, 16)
        copies.append(pltpu.make_async_copy(part, out.at[pl.ds(first + lo, part.shape[0])], sems.at[side]))
    run(copies)


def put(shard, step, lo, rows, n, gate, up, outs):
    return pl.pallas_call(
        functools.partial(put_kernel, step, lo, rows, n),
        in_specs=[SCALARS, WHOLE, WHOLE, OUTSIDE, OUTSIDE],
        out_specs=[OUTSIDE] * 2,
        out_shape=[jax.ShapeDtypeStruct(out.shape, out.dtype) for out in outs],
        scratch_shapes=[pltpu.SemaphoreType.DMA((2,))],
        input_output_aliases={3: 0, 4: 1},
        compiler_params=grant(4),
        name="put",
    )(shard, gate, up, *outs)


def add_kernel(count, *refs):
    terms = [ref[...] for ref in refs[:count]]
    while len(terms) > 1:
        terms = [terms[i] + terms[i + 1] for i in range(0, len(terms), 2)]
    refs[-1][...] = terms[0].astype(refs[-1].dtype)


def tree_add(terms, after, kind=jnp.float32):
    return pl.pallas_call(
        functools.partial(add_kernel, len(terms)),
        in_specs=[WHOLE] * len(terms) + [OUTSIDE] * len(after),
        out_specs=WHOLE,
        out_shape=jax.ShapeDtypeStruct(terms[0].shape, kind),
        compiler_params=grant(2),
        name="tree_add",
    )(*terms, *after)


def slot_kernel(count, index_ref, train, step, out):
    value = (train[...] + step[...]).astype(jnp.bfloat16).astype(jnp.float32)
    width = value.shape[1]
    value = jnp.concatenate([value] * count, axis=1)
    slot = lax.broadcasted_iota(jnp.int32, value.shape, 1) // width
    out[...] = jnp.where(slot == index_ref[0], value, 0.0)


def slot_of(index, train, step, count):
    return pl.pallas_call(
        functools.partial(slot_kernel, count),
        in_specs=[SCALARS, WHOLE, WHOLE],
        out_specs=WHOLE,
        out_shape=jax.ShapeDtypeStruct((1, count * train.shape[1]), jnp.float32),
        compiler_params=grant(2),
        name="slot",
    )(index, train, step)


def stages_of(n, most):
    bits = [1 << b for b in range(n.bit_length() - 1)]
    stages, bits = [bits[:1]], bits[1:]
    while bits:
        stages.append(bits[:most])
        bits = bits[most:]
    spans = []
    for stage in stages:
        masks = [0]
        for bit in stage:
            masks += [mask + bit for mask in masks]
        spans.append(masks[1:])
    return spans


def exchange(value, axis, n, masks, after=(), kind=jnp.float32):
    others = [lax.ppermute(value, axis, [(i, i ^ m) for i in range(n)]) for m in masks]
    return tree_add([value] + others, after, kind)


def shards(mesh, one_gate, other_gate, one_up, other_up, mix_share, norm_train, norm_step):
    n, t = mesh.shape["shard"], mesh.shape["tp"]
    me = lax.axis_index("shard")
    shard = me[None].astype(jnp.int32)
    device = shard * t + lax.axis_index("tp").astype(jnp.int32)
    rows, _ = one_gate.shape
    order = ring_order(n)
    forward = [(order[i], order[(i + 1) % n]) for i in range(n)]
    backward = [(b, a) for a, b in forward]
    spans = cuts(rows)
    fresh_gate, fresh_up, total = sums_of(mix_share[None], one_gate, other_gate, one_up, other_up)
    for masks in stages_of(n, 2):
        total = exchange(total, "shard", n, masks)
    factor_gate, factor_up, gate, up = narrow(spans, fresh_gate, fresh_up, total)
    outs = start_outputs(shard, spans, gate, up, n)
    norm = slot_of(device, norm_train[None], norm_step[None], n * t)
    left = [("tp", t, masks) for masks in stages_of(t, 1)] + [("shard", n, masks) for masks in stages_of(n, 1)]
    stage = 0
    for step in range(1, n):
        for c, (lo, hi) in enumerate(spans):
            gate[c] = lax.ppermute(gate[c], "shard", forward)
            up[c] = lax.ppermute(up[c], "shard", backward)
            outs = put(shard, step, lo, rows, n, gate[c], up[c], outs)
        if step > 1 and stage < len(left):
            norm = exchange(norm, *left[stage], (gate[0],))
            stage += 1
    for axis, size, masks in left[stage:]:
        norm = exchange(norm, axis, size, masks)
    serve_norm = norm[0].astype(jnp.bfloat16)
    return (outs[0], outs[1], factor_gate[0], factor_up[0], serve_norm)


def solution(mesh):
    def layer(*args):
        return shards(mesh, *args)

    return jax.shard_map(
        layer,
        mesh=mesh,
        in_specs=(
            P("shard", "tp"),
            P("shard", "tp"),
            P("shard", "tp"),
            P("shard", "tp"),
            P("shard"),
            P(("shard", "tp")),
            P(("shard", "tp")),
        ),
        out_specs=(P(None, "tp"), P(None, "tp"), P("tp"), P("tp"), P()),
        check_vma=False,
    )
```

```python
import functools

import jax
import jax.numpy as jnp
from jax import lax
from jax.experimental import pallas as pl
from jax.experimental.pallas import tpu as pltpu
from jax.sharding import PartitionSpec as P

WHOLE = pl.BlockSpec(memory_space=pltpu.VMEM)
OUTSIDE = pl.BlockSpec(memory_space=pl.ANY)
GRANT = 48
MOST = 1


def grant(mib):
    return pltpu.CompilerParams(vmem_limit_bytes=int(mib * 2**20))


def ring_order(n):
    return list(range(0, n, 2)) + list(range(1, n, 2))[::-1]


def ring_neighbour(shard, distance, n):
    place = lax.rem(jnp.where(lax.rem(shard, 2) == 0, shard // 2, n - 1 - shard // 2) + distance + n, n)
    return jnp.where(place < n - n // 2, 2 * place, 2 * (n - 1 - place) + 1)


def cuts(rows):
    if rows < 256:
        return [(0, rows)]
    edges = [0, 5 * rows // 8, rows]
    return list(zip(edges[:-1], edges[1:]))


def sums_kernel(pieces, share, one_g, other_g, one_u, other_u, fresh_g, fresh_u, sums, held, shares, sems, share_sem):
    rows, cols = fresh_g.shape
    tall = rows // pieces
    sources = (one_g, other_g, one_u, other_u)

    def copy(k, p):
        span = pl.ds(p * tall, tall)
        return pltpu.make_async_copy(sources[k].at[span], held.at[k, span], sems.at[k, p])

    first = pltpu.make_async_copy(share, shares, share_sem)
    first.start()
    for p in range(pieces):
        for k in range(4):
            copy(k, p).start()
    first.wait()
    row = lax.broadcasted_iota(jnp.int32, (rows, rows), 0)
    lane = lax.broadcasted_iota(jnp.int32, (rows, rows), 1)
    mix = jnp.sum(jnp.where(row == lane, shares[...], 0.0), axis=1, keepdims=True)
    rest = 1.0 - mix
    total = [jnp.zeros((8, cols), jnp.float32) for _ in range(2)]
    for p in range(pieces):
        for k in range(4):
            copy(k, p).wait()
        for r in range(p * tall, (p + 1) * tall, 8):
            m, w = mix[r:r + 8], rest[r:r + 8]
            for side, fresh in ((0, fresh_g), (1, fresh_u)):
                value = m * held[2 * side, r:r + 8] + w * held[2 * side + 1, r:r + 8]
                fresh[r:r + 8] = value
                total[side] = total[side] + value * value
    sums[0:1] = jnp.sum(total[0], axis=0, keepdims=True)
    sums[1:2] = jnp.sum(total[1], axis=0, keepdims=True)


def sums_of(share, one_gate, other_gate, one_up, other_up):
    rows, cols = one_gate.shape
    pieces = max(1, rows // 32)
    wide = jax.ShapeDtypeStruct((rows, cols), jnp.float32)
    return pl.pallas_call(
        functools.partial(sums_kernel, pieces),
        in_specs=[OUTSIDE] * 5,
        out_specs=[WHOLE] * 3,
        out_shape=[wide, wide, jax.ShapeDtypeStruct((2, cols), jnp.float32)],
        scratch_shapes=[
            pltpu.VMEM((4, rows, cols), jnp.float32),
            pltpu.VMEM(share.shape, jnp.float32),
            pltpu.SemaphoreType.DMA((4, pieces)),
            pltpu.SemaphoreType.DMA,
        ],
        compiler_params=grant(GRANT),
        name="sums",
    )(*[pltpu.with_memory_space_constraint(part, pltpu.HBM) for part in (share, one_gate, other_gate, one_up, other_up)])


def narrow_kernel(spans, fresh_g, fresh_u, total_ref, *outs):
    for side, fresh in ((0, fresh_g), (1, fresh_u)):
        scale = 1.0 / jnp.sqrt(total_ref[side:side + 1])
        for (lo, hi), out in zip(spans, outs[side * len(spans):]):
            for r in range(lo, hi, 16):
                out[r - lo:r - lo + 16] = (fresh[r:r + 16] * scale).astype(jnp.bfloat16)


def narrow(spans, fresh_gate, fresh_up, total):
    cols = fresh_gate.shape[1]
    shapes = [jax.ShapeDtypeStruct((hi - lo, cols), jnp.bfloat16) for lo, hi in spans]
    pieces = pl.pallas_call(
        functools.partial(narrow_kernel, spans),
        in_specs=[WHOLE] * 3,
        out_specs=[WHOLE] * (2 * len(spans)),
        out_shape=shapes * 2,
        compiler_params=grant(16),
        name="narrow",
    )(fresh_gate, fresh_up, total)
    return list(pieces[:len(spans)]), list(pieces[len(spans):])


def root_kernel(total_ref, factor_g, factor_u):
    factor_g[...] = jnp.sqrt(total_ref[0:1])
    factor_u[...] = jnp.sqrt(total_ref[1:2])


def roots(total):
    shape = jax.ShapeDtypeStruct((1, total.shape[1]), jnp.float32)
    return pl.pallas_call(
        root_kernel,
        in_specs=[WHOLE],
        out_specs=[WHOLE] * 2,
        out_shape=[shape, shape],
        compiler_params=grant(2),
        name="roots",
    )(total)


def run(copies):
    for copy in copies:
        copy.start()
    for copy in copies:
        copy.wait()


def start_kernel(spans, *refs):
    count = len(spans)
    outs, sems = refs[2 * count:2 * count + 2], refs[-1]
    first = pl.multiple_of(lax.axis_index("shard") * spans[-1][1], 16)
    run([
        pltpu.make_async_copy(refs[side * count + c], outs[side].at[pl.ds(first + lo, hi - lo)], sems.at[side, c])
        for side in range(2)
        for c, (lo, hi) in enumerate(spans)
    ])


def start_outputs(spans, gate, up, n):
    shape = jax.ShapeDtypeStruct((n * spans[-1][1], gate[0].shape[1]), jnp.bfloat16)
    return pl.pallas_call(
        functools.partial(start_kernel, spans),
        in_specs=[WHOLE] * (2 * len(spans)),
        out_specs=[OUTSIDE] * 2,
        out_shape=[shape, shape],
        scratch_shapes=[pltpu.SemaphoreType.DMA((2, len(spans)))],
        compiler_params=grant(4),
        name="start_outputs",
    )(*gate, *up)


def put_kernel(step, lo, rows, n, gate, up, _, __, out_g, out_u, sems):
    copies = []
    for side, (part, out, back) in enumerate(((gate, out_g, -step), (up, out_u, step))):
        first = pl.multiple_of(ring_neighbour(lax.axis_index("shard"), back, n) * rows, 16)
        copies.append(pltpu.make_async_copy(part, out.at[pl.ds(first + lo, part.shape[0])], sems.at[side]))
    run(copies)


def put(step, lo, rows, n, gate, up, outs):
    return pl.pallas_call(
        functools.partial(put_kernel, step, lo, rows, n),
        in_specs=[WHOLE, WHOLE, OUTSIDE, OUTSIDE],
        out_specs=[OUTSIDE] * 2,
        out_shape=[jax.ShapeDtypeStruct(out.shape, out.dtype) for out in outs],
        scratch_shapes=[pltpu.SemaphoreType.DMA((2,))],
        input_output_aliases={2: 0, 3: 1},
        compiler_params=grant(4),
        name="put",
    )(gate, up, *outs)


def add_kernel(count, *refs):
    terms = [ref[...] for ref in refs[:count]]
    while len(terms) > 1:
        terms = [terms[i] + terms[i + 1] for i in range(0, len(terms), 2)]
    refs[-1][...] = terms[0].astype(refs[-1].dtype)


def tree_add(terms, after, kind=jnp.float32):
    return pl.pallas_call(
        functools.partial(add_kernel, len(terms)),
        in_specs=[WHOLE] * len(terms) + [OUTSIDE] * len(after),
        out_specs=WHOLE,
        out_shape=jax.ShapeDtypeStruct(terms[0].shape, kind),
        compiler_params=grant(2),
        name="tree_add",
    )(*terms, *after)


def slot_kernel(count, t, train, step, out):
    value = (train[...] + step[...]).astype(jnp.bfloat16).astype(jnp.float32)
    width = value.shape[1]
    value = jnp.concatenate([value] * count, axis=1)
    slot = lax.broadcasted_iota(jnp.int32, value.shape, 1) // width
    out[...] = jnp.where(slot == lax.axis_index("shard") * t + lax.axis_index("tp"), value, 0.0)


def slot_of(train, step, count, t):
    return pl.pallas_call(
        functools.partial(slot_kernel, count, t),
        in_specs=[WHOLE, WHOLE],
        out_specs=WHOLE,
        out_shape=jax.ShapeDtypeStruct((1, count * train.shape[1]), jnp.float32),
        compiler_params=grant(2),
        name="slot",
    )(train, step)


def stages_of(n, most):
    bits = [1 << b for b in range(n.bit_length() - 1)]
    stages, bits = [bits[:1]], bits[1:]
    while bits:
        stages.append(bits[:most])
        bits = bits[most:]
    spans = []
    for stage in stages:
        masks = [0]
        for bit in stage:
            masks += [mask + bit for mask in masks]
        spans.append(masks[1:])
    return spans


def exchange(value, axis, n, masks, after=(), kind=jnp.float32):
    others = [lax.ppermute(value, axis, [(i, i ^ m) for i in range(n)]) for m in masks]
    return tree_add([value] + others, after, kind)


def shards(mesh, one_gate, other_gate, one_up, other_up, mix_share, norm_train, norm_step):
    n, t = mesh.shape["shard"], mesh.shape["tp"]
    rows, _ = one_gate.shape
    order = ring_order(n)
    forward = [(order[i], order[(i + 1) % n]) for i in range(n)]
    backward = [(b, a) for a, b in forward]
    spans = cuts(rows)
    fresh_gate, fresh_up, total = sums_of(mix_share[None], one_gate, other_gate, one_up, other_up)
    for masks in stages_of(n, MOST):
        total = exchange(total, "shard", n, masks)
    gate, up = narrow(spans, fresh_gate, fresh_up, total)
    factor_gate, factor_up = roots(total)
    outs = start_outputs(spans, gate, up, n)
    norm = slot_of(norm_train[None], norm_step[None], n * t, t)
    left = [("tp", t, masks) for masks in stages_of(t, 1)] + [("shard", n, masks) for masks in stages_of(n, 1)]
    stage = 0
    for step in range(1, n):
        for c, (lo, hi) in enumerate(spans):
            gate[c] = lax.ppermute(gate[c], "shard", forward)
            up[c] = lax.ppermute(up[c], "shard", backward)
            outs = put(step, lo, rows, n, gate[c], up[c], outs)
        if step > 1 and stage < len(left):
            norm = exchange(norm, *left[stage], (gate[0],))
            stage += 1
    for axis, size, masks in left[stage:]:
        norm = exchange(norm, axis, size, masks)
    serve_norm = norm[0].astype(jnp.bfloat16)
    return (outs[0], outs[1], factor_gate[0], factor_up[0], serve_norm)


def solution(mesh):
    def layer(*args):
        return shards(mesh, *args)

    return jax.shard_map(
        layer,
        mesh=mesh,
        in_specs=(
            P("shard", "tp"),
            P("shard", "tp"),
            P("shard", "tp"),
            P("shard", "tp"),
            P("shard"),
            P(("shard", "tp")),
            P(("shard", "tp")),
        ),
        out_specs=(P(None, "tp"), P(None, "tp"), P("tp"), P("tp"), P()),
        check_vma=False,
    )
```

```python
import functools

import jax
import jax.numpy as jnp
from jax import lax
from jax.experimental import pallas as pl
from jax.experimental.pallas import tpu as pltpu
from jax.sharding import PartitionSpec as P

WHOLE = pl.BlockSpec(memory_space=pltpu.VMEM)
OUTSIDE = pl.BlockSpec(memory_space=pl.ANY)
GRANT = 48
MOST = 2


def grant(mib):
    return pltpu.CompilerParams(vmem_limit_bytes=int(mib * 2**20))


def ring_order(n):
    return list(range(0, n, 2)) + list(range(1, n, 2))[::-1]


def ring_neighbour(shard, distance, n):
    place = lax.rem(jnp.where(lax.rem(shard, 2) == 0, shard // 2, n - 1 - shard // 2) + distance + n, n)
    return jnp.where(place < n - n // 2, 2 * place, 2 * (n - 1 - place) + 1)


def cuts(rows):
    if rows < 256:
        return [(0, rows)]
    edges = [0, rows // 2, 3 * rows // 4, rows]
    return list(zip(edges[:-1], edges[1:]))


def sums_kernel(edges, share, one_g, other_g, one_u, other_u, fresh_g, fresh_u, sums, held, shares, sems, share_sem):
    rows, cols = fresh_g.shape
    spans = list(zip(edges[:-1], edges[1:]))
    first = pltpu.make_async_copy(share, shares, share_sem)
    first.start()
    for p, (lo, hi) in enumerate(spans):
        for k, source in enumerate((one_g, other_g, one_u, other_u)):
            pltpu.make_async_copy(source.at[pl.ds(lo, hi - lo)], held.at[k, pl.ds(lo, hi - lo)], sems.at[p]).start()
    first.wait()
    row = lax.broadcasted_iota(jnp.int32, (rows, rows), 0)
    lane = lax.broadcasted_iota(jnp.int32, (rows, rows), 1)
    mix = jnp.sum(jnp.where(row == lane, shares[...], 0.0), axis=1, keepdims=True)
    rest = 1.0 - mix
    total = [jnp.zeros((8, cols), jnp.float32) for _ in range(2)]
    for p, (lo, hi) in enumerate(spans):
        piece = held.at[:, pl.ds(lo, hi - lo)]
        pltpu.make_async_copy(piece, piece, sems.at[p]).wait()
        for r in range(lo, hi, 8):
            m, w = mix[r:r + 8], rest[r:r + 8]
            for side, fresh in ((0, fresh_g), (1, fresh_u)):
                value = m * held[2 * side, r:r + 8] + w * held[2 * side + 1, r:r + 8]
                fresh[r:r + 8] = value
                total[side] = total[side] + value * value
    sums[0:1] = jnp.sum(total[0], axis=0, keepdims=True)
    sums[1:2] = jnp.sum(total[1], axis=0, keepdims=True)


def sums_of(share, one_gate, other_gate, one_up, other_up):
    rows, cols = one_gate.shape
    edges = [0, rows] if rows < 256 else [0, rows // 4, rows // 2, 3 * rows // 4, rows]
    wide = jax.ShapeDtypeStruct((rows, cols), jnp.float32)
    return pl.pallas_call(
        functools.partial(sums_kernel, edges),
        in_specs=[OUTSIDE] * 5,
        out_specs=[WHOLE] * 3,
        out_shape=[wide, wide, jax.ShapeDtypeStruct((2, cols), jnp.float32)],
        scratch_shapes=[
            pltpu.VMEM((4, rows, cols), jnp.float32),
            pltpu.VMEM(share.shape, jnp.float32),
            pltpu.SemaphoreType.DMA((len(edges) - 1,)),
            pltpu.SemaphoreType.DMA,
        ],
        compiler_params=grant(GRANT),
        name="sums",
    )(*[pltpu.with_memory_space_constraint(part, pltpu.HBM) for part in (share, one_gate, other_gate, one_up, other_up)])


def narrow_kernel(spans, fresh_g, fresh_u, total_ref, *outs):
    for side, fresh in ((0, fresh_g), (1, fresh_u)):
        scale = 1.0 / jnp.sqrt(total_ref[side:side + 1])
        for (lo, hi), out in zip(spans, outs[side * len(spans):]):
            for r in range(lo, hi, 16):
                out[r - lo:r - lo + 16] = (fresh[r:r + 16] * scale).astype(jnp.bfloat16)


def narrow(spans, fresh_gate, fresh_up, total):
    cols = fresh_gate.shape[1]
    shapes = [jax.ShapeDtypeStruct((hi - lo, cols), jnp.bfloat16) for lo, hi in spans]
    pieces = pl.pallas_call(
        functools.partial(narrow_kernel, spans),
        in_specs=[WHOLE] * 3,
        out_specs=[WHOLE] * (2 * len(spans)),
        out_shape=shapes * 2,
        compiler_params=grant(16),
        name="narrow",
    )(fresh_gate, fresh_up, total)
    return list(pieces[:len(spans)]), list(pieces[len(spans):])


def root_kernel(total_ref, factor_g, factor_u):
    factor_g[...] = jnp.sqrt(total_ref[0:1])
    factor_u[...] = jnp.sqrt(total_ref[1:2])


def roots(total):
    shape = jax.ShapeDtypeStruct((1, total.shape[1]), jnp.float32)
    return pl.pallas_call(
        root_kernel,
        in_specs=[WHOLE],
        out_specs=[WHOLE] * 2,
        out_shape=[shape, shape],
        compiler_params=grant(2),
        name="roots",
    )(total)


def run(copies):
    for copy in copies:
        copy.start()
    for copy in copies:
        copy.wait()


def start_kernel(spans, *refs):
    count = len(spans)
    outs, sems = refs[2 * count:2 * count + 2], refs[-1]
    first = pl.multiple_of(lax.axis_index("shard") * spans[-1][1], 16)
    run([
        pltpu.make_async_copy(refs[side * count + c], outs[side].at[pl.ds(first + lo, hi - lo)], sems.at[side, c])
        for side in range(2)
        for c, (lo, hi) in enumerate(spans)
    ])


def start_outputs(spans, gate, up, n):
    shape = jax.ShapeDtypeStruct((n * spans[-1][1], gate[0].shape[1]), jnp.bfloat16)
    return pl.pallas_call(
        functools.partial(start_kernel, spans),
        in_specs=[WHOLE] * (2 * len(spans)),
        out_specs=[OUTSIDE] * 2,
        out_shape=[shape, shape],
        scratch_shapes=[pltpu.SemaphoreType.DMA((2, len(spans)))],
        compiler_params=grant(4),
        name="start_outputs",
    )(*gate, *up)


def put_kernel(step, lo, rows, n, gate, up, _, __, out_g, out_u, sems):
    copies = []
    for side, (part, out, back) in enumerate(((gate, out_g, -step), (up, out_u, step))):
        first = pl.multiple_of(ring_neighbour(lax.axis_index("shard"), back, n) * rows, 16)
        copies.append(pltpu.make_async_copy(part, out.at[pl.ds(first + lo, part.shape[0])], sems.at[side]))
    run(copies)


def put(step, lo, rows, n, gate, up, outs):
    return pl.pallas_call(
        functools.partial(put_kernel, step, lo, rows, n),
        in_specs=[WHOLE, WHOLE, OUTSIDE, OUTSIDE],
        out_specs=[OUTSIDE] * 2,
        out_shape=[jax.ShapeDtypeStruct(out.shape, out.dtype) for out in outs],
        scratch_shapes=[pltpu.SemaphoreType.DMA((2,))],
        input_output_aliases={2: 0, 3: 1},
        compiler_params=grant(4),
        name="put",
    )(gate, up, *outs)


def add_kernel(count, *refs):
    terms = [ref[...] for ref in refs[:count]]
    while len(terms) > 1:
        terms = [terms[i] + terms[i + 1] for i in range(0, len(terms), 2)]
    refs[-1][...] = terms[0].astype(refs[-1].dtype)


def tree_add(terms, after, kind=jnp.float32):
    return pl.pallas_call(
        functools.partial(add_kernel, len(terms)),
        in_specs=[WHOLE] * len(terms) + [OUTSIDE] * len(after),
        out_specs=WHOLE,
        out_shape=jax.ShapeDtypeStruct(terms[0].shape, kind),
        compiler_params=grant(2),
        name="tree_add",
    )(*terms, *after)


def slot_kernel(count, t, train, step, out):
    value = (train[...] + step[...]).astype(jnp.bfloat16).astype(jnp.float32)
    width = value.shape[1]
    value = jnp.concatenate([value] * count, axis=1)
    slot = lax.broadcasted_iota(jnp.int32, value.shape, 1) // width
    out[...] = jnp.where(slot == lax.axis_index("shard") * t + lax.axis_index("tp"), value, 0.0)


def slot_of(train, step, count, t):
    return pl.pallas_call(
        functools.partial(slot_kernel, count, t),
        in_specs=[WHOLE, WHOLE],
        out_specs=WHOLE,
        out_shape=jax.ShapeDtypeStruct((1, count * train.shape[1]), jnp.float32),
        compiler_params=grant(2),
        name="slot",
    )(train, step)


def stages_of(n, most):
    bits = [1 << b for b in range(n.bit_length() - 1)]
    stages, bits = [bits[:1]], bits[1:]
    while bits:
        stages.append(bits[:most])
        bits = bits[most:]
    spans = []
    for stage in stages:
        masks = [0]
        for bit in stage:
            masks += [mask + bit for mask in masks]
        spans.append(masks[1:])
    return spans


def exchange(value, axis, n, masks, after=()):
    others = []
    for mask in masks:
        others.append(lax.ppermute(value, axis, [(i, i ^ mask) for i in range(n)]))
    return tree_add([value] + others, after)


def shards(mesh, one_gate, other_gate, one_up, other_up, mix_share, norm_train, norm_step):
    n, t = mesh.shape["shard"], mesh.shape["tp"]
    rows, _ = one_gate.shape
    order = ring_order(n)
    forward = [(order[i], order[(i + 1) % n]) for i in range(n)]
    backward = [(b, a) for a, b in forward]
    spans = cuts(rows)
    fresh_gate, fresh_up, total = sums_of(mix_share[None], one_gate, other_gate, one_up, other_up)
    norm = slot_of(norm_train[None], norm_step[None], n * t, t)
    for masks in stages_of(n, MOST):
        total = exchange(total, "shard", n, masks)
    gate, up = narrow(spans, fresh_gate, fresh_up, total)
    factor_gate, factor_up = roots(total)
    outs = start_outputs(spans, gate, up, n)
    left = [("tp", t, masks) for masks in stages_of(t, 1)] + [("shard", n, masks) for masks in stages_of(n, 1)]
    norm = exchange(norm, *left[0])
    stage = 1
    for step in range(1, n):
        for c, (lo, hi) in enumerate(spans):
            gate[c] = lax.ppermute(gate[c], "shard", forward)
            up[c] = lax.ppermute(up[c], "shard", backward)
            outs = put(step, lo, rows, n, gate[c], up[c], outs)
        if stage < len(left):
            norm = exchange(norm, *left[stage], (gate[0],))
            stage += 1
    for axis, size, masks in left[stage:]:
        norm = exchange(norm, axis, size, masks)
    serve_norm = norm[0].astype(jnp.bfloat16)
    return (outs[0], outs[1], factor_gate[0], factor_up[0], serve_norm)


def solution(mesh):
    def layer(*args):
        return shards(mesh, *args)

    return jax.shard_map(
        layer,
        mesh=mesh,
        in_specs=(
            P("shard", "tp"),
            P("shard", "tp"),
            P("shard", "tp"),
            P("shard", "tp"),
            P("shard"),
            P(("shard", "tp")),
            P(("shard", "tp")),
        ),
        out_specs=(P(None, "tp"), P(None, "tp"), P("tp"), P("tp"), P()),
        check_vma=False,
    )
```

```python
import functools

import jax
import jax.numpy as jnp
from jax import lax
from jax.experimental import pallas as pl
from jax.experimental.pallas import tpu as pltpu
from jax.sharding import PartitionSpec as P

WHOLE = pl.BlockSpec(memory_space=pltpu.VMEM)
OUTSIDE = pl.BlockSpec(memory_space=pl.ANY)
GRANT = 47
EARLY = 16
MOST = 2


def grant(mib):
    return pltpu.CompilerParams(vmem_limit_bytes=int(mib * 2**20))


def ring_order(n):
    return list(range(0, n, 2)) + list(range(1, n, 2))[::-1]


def ring_neighbour(shard, distance, n):
    place = lax.rem(jnp.where(lax.rem(shard, 2) == 0, shard // 2, n - 1 - shard // 2) + distance + n, n)
    return jnp.where(place < n - n // 2, 2 * place, 2 * (n - 1 - place) + 1)


def cuts(rows):
    if rows < 256:
        return [(0, rows)]
    edges = [0, EARLY, EARLY + 16 * ((rows - EARLY) // 32), rows]
    return list(zip(edges[:-1], edges[1:]))


def sums_kernel(edges, share, one_g, other_g, one_u, other_u, fresh_g, fresh_u, sums, *refs):
    early, (held, shares, sems, share_sem) = refs[:-4], refs[-4:]
    rows, cols = fresh_g.shape
    spans = list(zip(edges[:-1], edges[1:]))
    first = pltpu.make_async_copy(share, shares, share_sem)
    first.start()
    for p, (lo, hi) in enumerate(spans):
        for k, source in enumerate((one_g, other_g, one_u, other_u)):
            pltpu.make_async_copy(source.at[pl.ds(lo, hi - lo)], held.at[k, pl.ds(lo, hi - lo)], sems.at[p]).start(priority=k % 2)
    first.wait()
    row = lax.broadcasted_iota(jnp.int32, (rows, rows), 0)
    lane = lax.broadcasted_iota(jnp.int32, (rows, rows), 1)
    mix = jnp.sum(jnp.where(row == lane, shares[...], 0.0), axis=1, keepdims=True)
    rest = 1.0 - mix
    total = [jnp.zeros((8, cols), jnp.float32) for _ in range(2)]
    for p, (lo, hi) in enumerate(spans):
        piece = held.at[:, pl.ds(lo, hi - lo)]
        pltpu.make_async_copy(piece, piece, sems.at[p]).wait()
        for r in range(lo, hi, 8):
            m, w = mix[r:r + 8], rest[r:r + 8]
            for side, fresh in ((0, fresh_g), (1, fresh_u)):
                value = m * held[2 * side, r:r + 8] + w * held[2 * side + 1, r:r + 8]
                fresh[r:r + 8] = value
                if early and r < early[side].shape[0]:
                    early[side][r:r + 8] = value
                total[side] = total[side] + value * value
    sums[0:1] = jnp.sum(total[0], axis=0, keepdims=True)
    sums[1:2] = jnp.sum(total[1], axis=0, keepdims=True)


def sums_of(share, one_gate, other_gate, one_up, other_up):
    rows, cols = one_gate.shape
    edges = [0, rows] if rows < 256 else [0, rows // 4, rows // 2, 3 * rows // 4, rows]
    wide = jax.ShapeDtypeStruct((rows, cols), jnp.float32)
    early = [jax.ShapeDtypeStruct((EARLY, cols), jnp.float32)] * 2 if rows >= 256 else []
    return pl.pallas_call(
        functools.partial(sums_kernel, edges),
        in_specs=[OUTSIDE] * 5,
        out_specs=[WHOLE] * (3 + len(early)),
        out_shape=[wide, wide, jax.ShapeDtypeStruct((2, cols), jnp.float32)] + early,
        scratch_shapes=[
            pltpu.VMEM((4, rows, cols), jnp.float32),
            pltpu.VMEM(share.shape, jnp.float32),
            pltpu.SemaphoreType.DMA((len(edges) - 1,)),
            pltpu.SemaphoreType.DMA,
        ],
        compiler_params=grant(GRANT),
        name="sums",
    )(*[pltpu.with_memory_space_constraint(part, pltpu.HBM) for part in (share, one_gate, other_gate, one_up, other_up)])


def narrow_kernel(spans, fresh_g, fresh_u, total_ref, *outs):
    for side, fresh in ((0, fresh_g), (1, fresh_u)):
        scale = 1.0 / jnp.sqrt(total_ref[side:side + 1])
        for (lo, hi), out in zip(spans, outs[side * len(spans):]):
            for r in range(lo, hi, 16):
                out[r - lo:r - lo + 16] = (fresh[r:r + 16] * scale).astype(jnp.bfloat16)


def narrow(spans, fresh_gate, fresh_up, total):
    cols = fresh_gate.shape[1]
    shapes = [jax.ShapeDtypeStruct((hi - lo, cols), jnp.bfloat16) for lo, hi in spans]
    pieces = pl.pallas_call(
        functools.partial(narrow_kernel, spans),
        in_specs=[WHOLE] * 3,
        out_specs=[WHOLE] * (2 * len(spans)),
        out_shape=shapes * 2,
        compiler_params=grant(16),
        name="narrow",
    )(fresh_gate, fresh_up, total)
    return list(pieces[:len(spans)]), list(pieces[len(spans):])


def late_kernel(early_g, early_u, total_ref, gate, up):
    for side, early, out in ((0, early_g, gate), (1, early_u, up)):
        scale = 1.0 / jnp.sqrt(total_ref[side:side + 1])
        for r in range(0, out.shape[0], 16):
            out[r:r + 16] = (early[r:r + 16] * scale).astype(jnp.bfloat16)


def narrow_late(early_gate, early_up, total):
    shape = jax.ShapeDtypeStruct(early_gate.shape, jnp.bfloat16)
    return pl.pallas_call(
        late_kernel,
        in_specs=[WHOLE] * 3,
        out_specs=[WHOLE] * 2,
        out_shape=[shape, shape],
        compiler_params=grant(4),
        name="narrow_late",
    )(early_gate, early_up, total)


def root_kernel(total_ref, factor_g, factor_u):
    factor_g[...] = jnp.sqrt(total_ref[0:1])
    factor_u[...] = jnp.sqrt(total_ref[1:2])


def roots(total):
    shape = jax.ShapeDtypeStruct((1, total.shape[1]), jnp.float32)
    return pl.pallas_call(
        root_kernel,
        in_specs=[WHOLE],
        out_specs=[WHOLE] * 2,
        out_shape=[shape, shape],
        compiler_params=grant(2),
        name="roots",
    )(total)


def run(copies):
    for copy in copies:
        copy.start()
    for copy in copies:
        copy.wait()


def start_kernel(spans, *refs):
    count = len(spans)
    outs, sems = refs[2 * count:2 * count + 2], refs[-1]
    first = pl.multiple_of(lax.axis_index("shard") * spans[-1][1], 16)
    run([
        pltpu.make_async_copy(refs[side * count + c], outs[side].at[pl.ds(first + lo, hi - lo)], sems.at[side, c])
        for side in range(2)
        for c, (lo, hi) in enumerate(spans)
    ])


def start_outputs(spans, gate, up, n):
    shape = jax.ShapeDtypeStruct((n * spans[-1][1], gate[0].shape[1]), jnp.bfloat16)
    return pl.pallas_call(
        functools.partial(start_kernel, spans),
        in_specs=[WHOLE] * (2 * len(spans)),
        out_specs=[OUTSIDE] * 2,
        out_shape=[shape, shape],
        scratch_shapes=[pltpu.SemaphoreType.DMA((2, len(spans)))],
        compiler_params=grant(4),
        name="start_outputs",
    )(*gate, *up)


def put_kernel(step, lo, rows, n, gate, up, _, __, out_g, out_u, sems):
    copies = []
    for side, (part, out, back) in enumerate(((gate, out_g, -step), (up, out_u, step))):
        first = pl.multiple_of(ring_neighbour(lax.axis_index("shard"), back, n) * rows, 16)
        copies.append(pltpu.make_async_copy(part, out.at[pl.ds(first + lo, part.shape[0])], sems.at[side]))
    run(copies)


def put(step, lo, rows, n, gate, up, outs):
    return pl.pallas_call(
        functools.partial(put_kernel, step, lo, rows, n),
        in_specs=[WHOLE, WHOLE, OUTSIDE, OUTSIDE],
        out_specs=[OUTSIDE] * 2,
        out_shape=[jax.ShapeDtypeStruct(out.shape, out.dtype) for out in outs],
        scratch_shapes=[pltpu.SemaphoreType.DMA((2,))],
        input_output_aliases={2: 0, 3: 1},
        compiler_params=grant(4),
        name="put",
    )(gate, up, *outs)


def add_kernel(count, *refs):
    terms = [ref[...] for ref in refs[:count]]
    while len(terms) > 1:
        terms = [terms[i] + terms[i + 1] for i in range(0, len(terms), 2)]
    refs[-1][...] = terms[0].astype(refs[-1].dtype)


def tree_add(terms, after, kind=jnp.float32):
    return pl.pallas_call(
        functools.partial(add_kernel, len(terms)),
        in_specs=[WHOLE] * len(terms) + [OUTSIDE] * len(after),
        out_specs=WHOLE,
        out_shape=jax.ShapeDtypeStruct(terms[0].shape, kind),
        compiler_params=grant(2),
        name="tree_add",
    )(*terms, *after)


def slot_kernel(count, t, train, step, out):
    value = (train[...] + step[...]).astype(jnp.bfloat16).astype(jnp.float32)
    width = value.shape[1]
    value = jnp.concatenate([value] * count, axis=1)
    slot = lax.broadcasted_iota(jnp.int32, value.shape, 1) // width
    out[...] = jnp.where(slot == lax.axis_index("shard") * t + lax.axis_index("tp"), value, 0.0)


def slot_of(train, step, count, t):
    return pl.pallas_call(
        functools.partial(slot_kernel, count, t),
        in_specs=[WHOLE, WHOLE],
        out_specs=WHOLE,
        out_shape=jax.ShapeDtypeStruct((1, count * train.shape[1]), jnp.float32),
        compiler_params=grant(2),
        name="slot",
    )(train, step)


def stages_of(n, most):
    bits = [1 << b for b in range(n.bit_length() - 1)]
    stages, bits = [bits[:1]], bits[1:]
    while bits:
        stages.append(bits[:most])
        bits = bits[most:]
    spans = []
    for stage in stages:
        masks = [0]
        for bit in stage:
            masks += [mask + bit for mask in masks]
        spans.append(masks[1:])
    return spans


def exchange(value, axis, n, masks, after=()):
    others = []
    for mask in masks:
        others.append(lax.ppermute(value, axis, [(i, i ^ mask) for i in range(n)]))
    return tree_add([value] + others, after)


def shards(mesh, one_gate, other_gate, one_up, other_up, mix_share, norm_train, norm_step):
    n, t = mesh.shape["shard"], mesh.shape["tp"]
    rows, _ = one_gate.shape
    order = ring_order(n)
    forward = [(order[i], order[(i + 1) % n]) for i in range(n)]
    backward = [(b, a) for a, b in forward]
    spans = cuts(rows)
    fresh_gate, fresh_up, total, *early = sums_of(mix_share[None], one_gate, other_gate, one_up, other_up)
    if early:
        early[0] = lax.ppermute(early[0], "shard", forward)
        early[1] = lax.ppermute(early[1], "shard", backward)
    norm = slot_of(norm_train[None], norm_step[None], n * t, t)
    for masks in stages_of(n, MOST):
        total = exchange(total, "shard", n, masks)
    gate, up = narrow(spans, fresh_gate, fresh_up, total)
    factor_gate, factor_up = roots(total)
    outs = start_outputs(spans, gate, up, n)
    left = [("tp", t, masks) for masks in stages_of(t, 1)]
    left = left[1:] + [("shard", n, masks) for masks in stages_of(n, 1)] + left[:1]
    stage = 0
    for step in range(1, n):
        for c, (lo, hi) in enumerate(spans):
            if early and (step, c) == (1, 0):
                gate[c], up[c] = narrow_late(*early, total)
            else:
                gate[c] = lax.ppermute(gate[c], "shard", forward)
                up[c] = lax.ppermute(up[c], "shard", backward)
            outs = put(step, lo, rows, n, gate[c], up[c], outs)
        if step > 1 and stage < len(left) - 1:
            norm = exchange(norm, *left[stage], (gate[0],))
            stage += 1
    for axis, size, masks in left[stage:]:
        norm = exchange(norm, axis, size, masks)
    serve_norm = norm[0].astype(jnp.bfloat16)
    return (outs[0], outs[1], factor_gate[0], factor_up[0], serve_norm)


def solution(mesh):
    def layer(*args):
        return shards(mesh, *args)

    return jax.shard_map(
        layer,
        mesh=mesh,
        in_specs=(
            P("shard", "tp"),
            P("shard", "tp"),
            P("shard", "tp"),
            P("shard", "tp"),
            P("shard"),
            P(("shard", "tp")),
            P(("shard", "tp")),
        ),
        out_specs=(P(None, "tp"), P(None, "tp"), P("tp"), P("tp"), P()),
        check_vma=False,
    )
```

```python
import functools

import jax
import jax.numpy as jnp
from jax import lax
from jax.experimental import pallas as pl
from jax.experimental.pallas import tpu as pltpu
from jax.sharding import PartitionSpec as P

WHOLE = pl.BlockSpec(memory_space=pltpu.VMEM)
OUTSIDE = pl.BlockSpec(memory_space=pl.ANY)
GRANT = 47
EARLY = 32
MOST = 2


def grant(mib):
    return pltpu.CompilerParams(vmem_limit_bytes=int(mib * 2**20))


def ring_order(n):
    return list(range(0, n, 2)) + list(range(1, n, 2))[::-1]


def ring_neighbour(shard, distance, n):
    place = lax.rem(jnp.where(lax.rem(shard, 2) == 0, shard // 2, n - 1 - shard // 2) + distance + n, n)
    return jnp.where(place < n - n // 2, 2 * place, 2 * (n - 1 - place) + 1)


def cuts(rows):
    if rows < 256:
        return [(0, rows)]
    edges = [0, EARLY, EARLY + 16 * ((rows - EARLY) // 32), rows]
    return list(zip(edges[:-1], edges[1:]))


def sums_kernel(edges, share, one_g, other_g, one_u, other_u, fresh_g, fresh_u, sums, *refs):
    early, (held, shares, sems, share_sem) = refs[:-4], refs[-4:]
    rows, cols = fresh_g.shape
    spans = list(zip(edges[:-1], edges[1:]))
    first = pltpu.make_async_copy(share, shares, share_sem)
    first.start()
    for p, (lo, hi) in enumerate(spans):
        for k, source in enumerate((one_g, other_g, one_u, other_u)):
            pltpu.make_async_copy(source.at[pl.ds(lo, hi - lo)], held.at[k, pl.ds(lo, hi - lo)], sems.at[p]).start(priority=k % 2)
    first.wait()
    row = lax.broadcasted_iota(jnp.int32, (rows, rows), 0)
    lane = lax.broadcasted_iota(jnp.int32, (rows, rows), 1)
    mix = jnp.sum(jnp.where(row == lane, shares[...], 0.0), axis=1, keepdims=True)
    rest = 1.0 - mix
    total = [jnp.zeros((8, cols), jnp.float32) for _ in range(2)]
    for p, (lo, hi) in enumerate(spans):
        piece = held.at[:, pl.ds(lo, hi - lo)]
        pltpu.make_async_copy(piece, piece, sems.at[p]).wait()
        for r in range(lo, hi, 8):
            m, w = mix[r:r + 8], rest[r:r + 8]
            for side, fresh in ((0, fresh_g), (1, fresh_u)):
                value = m * held[2 * side, r:r + 8] + w * held[2 * side + 1, r:r + 8]
                fresh[r:r + 8] = value
                if early and r < EARLY:
                    early[2 * (r // (EARLY // 2)) + side][r % (EARLY // 2):r % (EARLY // 2) + 8] = value
                total[side] = total[side] + value * value
    sums[0:1] = jnp.sum(total[0], axis=0, keepdims=True)
    sums[1:2] = jnp.sum(total[1], axis=0, keepdims=True)


def sums_of(share, one_gate, other_gate, one_up, other_up):
    rows, cols = one_gate.shape
    edges = [0, rows] if rows < 256 else [0, rows // 4, rows // 2, 3 * rows // 4, rows]
    wide = jax.ShapeDtypeStruct((rows, cols), jnp.float32)
    early = [jax.ShapeDtypeStruct((EARLY // 2, cols), jnp.float32)] * 4 if rows >= 256 else []
    return pl.pallas_call(
        functools.partial(sums_kernel, edges),
        in_specs=[OUTSIDE] * 5,
        out_specs=[WHOLE] * (3 + len(early)),
        out_shape=[wide, wide, jax.ShapeDtypeStruct((2, cols), jnp.float32)] + early,
        scratch_shapes=[
            pltpu.VMEM((4, rows, cols), jnp.float32),
            pltpu.VMEM(share.shape, jnp.float32),
            pltpu.SemaphoreType.DMA((len(edges) - 1,)),
            pltpu.SemaphoreType.DMA,
        ],
        compiler_params=grant(GRANT),
        name="sums",
    )(*[pltpu.with_memory_space_constraint(part, pltpu.HBM) for part in (share, one_gate, other_gate, one_up, other_up)])


def narrow_kernel(spans, fresh_g, fresh_u, total_ref, *outs):
    for side, fresh in ((0, fresh_g), (1, fresh_u)):
        scale = 1.0 / jnp.sqrt(total_ref[side:side + 1])
        for (lo, hi), out in zip(spans, outs[side * len(spans):]):
            for r in range(lo, hi, 16):
                out[r - lo:r - lo + 16] = (fresh[r:r + 16] * scale).astype(jnp.bfloat16)


def narrow(spans, fresh_gate, fresh_up, total):
    cols = fresh_gate.shape[1]
    shapes = [jax.ShapeDtypeStruct((hi - lo, cols), jnp.bfloat16) for lo, hi in spans]
    pieces = pl.pallas_call(
        functools.partial(narrow_kernel, spans),
        in_specs=[WHOLE] * 3,
        out_specs=[WHOLE] * (2 * len(spans)),
        out_shape=shapes * 2,
        compiler_params=grant(16),
        name="narrow",
    )(fresh_gate, fresh_up, total)
    return list(pieces[:len(spans)]), list(pieces[len(spans):])


def late_kernel(*refs):
    early, total_ref, outs = refs[:-3], refs[-3], refs[-2:]
    for side, out in enumerate(outs):
        scale = 1.0 / jnp.sqrt(total_ref[side:side + 1])
        low = 0
        for part in early[side::2]:
            tall = part.shape[0]
            out[low:low + tall] = (part[...] * scale).astype(jnp.bfloat16)
            low += tall


def narrow_late(early, total):
    shape = jax.ShapeDtypeStruct((EARLY, total.shape[1]), jnp.bfloat16)
    return pl.pallas_call(
        late_kernel,
        in_specs=[WHOLE] * (len(early) + 1),
        out_specs=[WHOLE] * 2,
        out_shape=[shape, shape],
        compiler_params=grant(4),
        name="narrow_late",
    )(*early, total)


def root_kernel(total_ref, factor_g, factor_u):
    factor_g[...] = jnp.sqrt(total_ref[0:1])
    factor_u[...] = jnp.sqrt(total_ref[1:2])


def roots(total):
    shape = jax.ShapeDtypeStruct((1, total.shape[1]), jnp.float32)
    return pl.pallas_call(
        root_kernel,
        in_specs=[WHOLE],
        out_specs=[WHOLE] * 2,
        out_shape=[shape, shape],
        compiler_params=grant(2),
        name="roots",
    )(total)


def run(copies):
    for copy in copies:
        copy.start()
    for copy in copies:
        copy.wait()


def start_kernel(spans, *refs):
    count = len(spans)
    outs, sems = refs[2 * count:2 * count + 2], refs[-1]
    first = pl.multiple_of(lax.axis_index("shard") * spans[-1][1], 16)
    run([
        pltpu.make_async_copy(refs[side * count + c], outs[side].at[pl.ds(first + lo, hi - lo)], sems.at[side, c])
        for side in range(2)
        for c, (lo, hi) in enumerate(spans)
    ])


def start_outputs(spans, gate, up, n):
    shape = jax.ShapeDtypeStruct((n * spans[-1][1], gate[0].shape[1]), jnp.bfloat16)
    return pl.pallas_call(
        functools.partial(start_kernel, spans),
        in_specs=[WHOLE] * (2 * len(spans)),
        out_specs=[OUTSIDE] * 2,
        out_shape=[shape, shape],
        scratch_shapes=[pltpu.SemaphoreType.DMA((2, len(spans)))],
        compiler_params=grant(4),
        name="start_outputs",
    )(*gate, *up)


def put_kernel(step, lo, rows, n, gate, up, _, __, out_g, out_u, sems):
    copies = []
    for side, (part, out, back) in enumerate(((gate, out_g, -step), (up, out_u, step))):
        first = pl.multiple_of(ring_neighbour(lax.axis_index("shard"), back, n) * rows, 16)
        copies.append(pltpu.make_async_copy(part, out.at[pl.ds(first + lo, part.shape[0])], sems.at[side]))
    run(copies)


def put(step, lo, rows, n, gate, up, outs):
    return pl.pallas_call(
        functools.partial(put_kernel, step, lo, rows, n),
        in_specs=[WHOLE, WHOLE, OUTSIDE, OUTSIDE],
        out_specs=[OUTSIDE] * 2,
        out_shape=[jax.ShapeDtypeStruct(out.shape, out.dtype) for out in outs],
        scratch_shapes=[pltpu.SemaphoreType.DMA((2,))],
        input_output_aliases={2: 0, 3: 1},
        compiler_params=grant(4),
        name="put",
    )(gate, up, *outs)


def add_kernel(count, *refs):
    terms = [ref[...] for ref in refs[:count]]
    while len(terms) > 1:
        terms = [terms[i] + terms[i + 1] for i in range(0, len(terms), 2)]
    refs[-1][...] = terms[0].astype(refs[-1].dtype)


def tree_add(terms, after, kind=jnp.float32):
    return pl.pallas_call(
        functools.partial(add_kernel, len(terms)),
        in_specs=[WHOLE] * len(terms) + [OUTSIDE] * len(after),
        out_specs=WHOLE,
        out_shape=jax.ShapeDtypeStruct(terms[0].shape, kind),
        compiler_params=grant(2),
        name="tree_add",
    )(*terms, *after)


def slot_kernel(count, t, train, step, out):
    value = (train[...] + step[...]).astype(jnp.bfloat16).astype(jnp.float32)
    width = value.shape[1]
    value = jnp.concatenate([value] * count, axis=1)
    slot = lax.broadcasted_iota(jnp.int32, value.shape, 1) // width
    out[...] = jnp.where(slot == lax.axis_index("shard") * t + lax.axis_index("tp"), value, 0.0)


def slot_of(train, step, count, t):
    return pl.pallas_call(
        functools.partial(slot_kernel, count, t),
        in_specs=[WHOLE, WHOLE],
        out_specs=WHOLE,
        out_shape=jax.ShapeDtypeStruct((1, count * train.shape[1]), jnp.float32),
        compiler_params=grant(2),
        name="slot",
    )(train, step)


def stages_of(n, most):
    bits = [1 << b for b in range(n.bit_length() - 1)]
    stages, bits = [bits[:1]], bits[1:]
    while bits:
        stages.append(bits[:most])
        bits = bits[most:]
    spans = []
    for stage in stages:
        masks = [0]
        for bit in stage:
            masks += [mask + bit for mask in masks]
        spans.append(masks[1:])
    return spans


def exchange(value, axis, n, masks, after=()):
    others = []
    for mask in masks:
        others.append(lax.ppermute(value, axis, [(i, i ^ mask) for i in range(n)]))
    return tree_add([value] + others, after)


def shards(mesh, one_gate, other_gate, one_up, other_up, mix_share, norm_train, norm_step):
    n, t = mesh.shape["shard"], mesh.shape["tp"]
    rows, _ = one_gate.shape
    order = ring_order(n)
    forward = [(order[i], order[(i + 1) % n]) for i in range(n)]
    backward = [(b, a) for a, b in forward]
    spans = cuts(rows)
    fresh_gate, fresh_up, total, *early = sums_of(mix_share[None], one_gate, other_gate, one_up, other_up)
    for k in range(len(early)):
        early[k] = lax.ppermute(early[k], "shard", backward if k % 2 else forward)
    norm = slot_of(norm_train[None], norm_step[None], n * t, t)
    for masks in stages_of(n, MOST):
        total = exchange(total, "shard", n, masks)
    gate, up = narrow(spans, fresh_gate, fresh_up, total)
    factor_gate, factor_up = roots(total)
    outs = start_outputs(spans, gate, up, n)
    left = [("tp", t, masks) for masks in stages_of(t, 1)]
    left = left[1:] + [("shard", n, masks) for masks in stages_of(n, 1)] + left[:1]
    stage = 0
    for step in range(1, n):
        for c, (lo, hi) in enumerate(spans):
            if early and (step, c) == (1, 0):
                gate[c], up[c] = narrow_late(early, total)
            else:
                gate[c] = lax.ppermute(gate[c], "shard", forward)
                up[c] = lax.ppermute(up[c], "shard", backward)
            outs = put(step, lo, rows, n, gate[c], up[c], outs)
        if step > 1 and stage < len(left) - 1:
            norm = exchange(norm, *left[stage], (gate[0],))
            stage += 1
    for axis, size, masks in left[stage:]:
        norm = exchange(norm, axis, size, masks)
    serve_norm = norm[0].astype(jnp.bfloat16)
    return (outs[0], outs[1], factor_gate[0], factor_up[0], serve_norm)


def solution(mesh):
    def layer(*args):
        return shards(mesh, *args)

    return jax.shard_map(
        layer,
        mesh=mesh,
        in_specs=(
            P("shard", "tp"),
            P("shard", "tp"),
            P("shard", "tp"),
            P("shard", "tp"),
            P("shard"),
            P(("shard", "tp")),
            P(("shard", "tp")),
        ),
        out_specs=(P(None, "tp"), P(None, "tp"), P("tp"), P("tp"), P()),
        check_vma=False,
    )
```
